256 devices in a mesh: section: 8 (over z), dp: 32 (over x, y, core).
Axes of the slice: x: 4, y: 4, z: 8, core: 2. Of those that a mesh axis runs over, the one named last changes fastest.
Arguments:
- inject: bfloat16 [8, 256, 4096], P('section', 'dp'), may hold values from -42 to 42, as said below
- w_gate: bfloat16 [8, 4096, 11008], P('section', None, 'dp'), may hold values from -0.09375 to 0.09375
- w_up: bfloat16 [8, 4096, 11008], P('section', None, 'dp'), may hold values from -0.09375 to 0.09375
- w_down: bfloat16 [8, 11008, 4096], P('section', 'dp'), may hold values from -0.0546875 to 0.0546875
- gain: float32 [8, 4096], P('section'), may hold values from 0.5 to 1.5
Outputs:
- iterate: float32 [8, 256, 4096], P('section', 'dp')
- mixing: float32 [8, 5, 5], P('section')
The draws below stay inside these ranges and needn't reach their ends.
Inputs may be any that keep to these rules, and one draw needn't show every extreme that they name: inject has entries of varied magnitude from token to token.
All inputs are finite; a program needn't handle non-finite values.
Results may differ from the reference program's by a relative error of at most 0.0038.
Values may be sent and summed in bfloat16 or wider, within the bound.
A program may use at most 64 MiB of HBM per device.

```python
import math
import jax
import jax.numpy as jnp
from jax import lax

D = 4096
FF = 11008
ITERS = 5
HIST = 5
SECTIONS = 8
TOKENS = 256
N_DP = 32


def draw_inject(key, part):
    first = jax.random.fold_in(key, 11)
    second = jax.random.fold_in(key, 12)
    ramp = 3.0 ** (jnp.arange(TOKENS, dtype=jnp.float32) / TOKENS)
    base = jnp.clip(jax.random.normal(first, (SECTIONS, TOKENS, D), jnp.float32), -4.0, 4.0)
    scales = jnp.exp(jax.random.uniform(second, (SECTIONS, TOKENS, 1), jnp.float32, math.log(0.3), math.log(3.0)))
    values = jnp.clip(base * ramp[None, :, None] * scales, -42.0, 42.0)
    values = values.at[0, TOKENS - 1, 0].set(42.0).at[0, TOKENS - 1, 1].set(-42.0)
    return values.astype(jnp.bfloat16)


def block_levels(rng, dims, pieces, low, largest):
    def one(dim, parts):
        steps = jax.random.uniform(jax.random.fold_in(jax.random.fold_in(rng, 6), dim), (parts,), jnp.float32, low / len(pieces), largest / len(pieces))
        return jnp.repeat(jnp.exp(steps), dims[dim] // parts).reshape((-1,) + (1,) * (len(dims) - dim - 1))

    factor_of = one(*pieces[0])
    for cut in pieces[1:]:
        factor_of = factor_of * one(*cut)
    return factor_of


def bell_draw(rng, shape, spread, limit, shards=(), kind=jnp.bfloat16):
    factor_of = block_levels(rng, shape, shards, -0.22, 0.18) if shards else 1.0
    values = jax.random.normal(rng, shape, jnp.float32) * spread * factor_of
    return jnp.minimum(jnp.maximum(values, -limit), limit).astype(kind)


def setup_inputs(seed: int = 0) -> dict:
    splits = jax.random.split(jax.random.key(seed), 6)
    return {
        "inject": draw_inject(jax.random.fold_in(splits[5], 71), 0),
        "w_gate": bell_draw(splits[1], (SECTIONS, D, FF), D ** -0.5, 0.09375, ((0, 8), (2, 32))),
        "w_up": bell_draw(splits[2], (SECTIONS, D, FF), D ** -0.5, 0.09375, ((0, 8), (2, 32))),
        "w_down": bell_draw(splits[3], (SECTIONS, FF, D), FF ** -0.5, 0.0546875, ((0, 8), (1, 32))),
        "gain": jnp.clip(1.0 + 0.1 * jax.random.normal(splits[4], (SECTIONS, D), jnp.float32), 0.5, 1.5),
    }


def rms_scaled(values, gain_row):
    inverse = lax.rsqrt(lax.optimization_barrier(jnp.mean(values * values, axis=-1, keepdims=True)) + 1e-06)
    return (values * inverse * gain_row).astype(jnp.bfloat16)

def solve_small(system, target):
    count = system.shape[-1]
    entries = [[system[..., i, j] for j in range(count)] for i in range(count)]
    values = [target[..., i] for i in range(count)]
    for p in range(count):
        for i in range(p + 1, count):
            factor = entries[i][p] / entries[p][p]
            for j in range(p, count):
                entries[i][j] = entries[i][j] - factor * entries[p][j]
            values[i] = values[i] - factor * values[p]
    answer = [None] * count
    for i in range(count - 1, -1, -1):
        accum = values[i]
        for j in range(i + 1, count):
            accum = accum - entries[i][j] * answer[j]
        answer[i] = accum / entries[i][i]
    return jnp.stack(answer, axis=-1)

def mixing_weights(matrix, iteration):
    live = (jnp.arange(HIST) <= iteration).astype(jnp.float32)
    damp = 0.01 * jnp.trace(matrix, axis1=-2, axis2=-1) / (iteration + 1) + 1e-06
    eye_mat = jnp.eye(HIST, dtype=jnp.float32)
    diagonal = live * damp[..., None] + (1.0 - live)
    system = matrix * live[:, None] * live[None, :] + eye_mat * diagonal[..., None, :]
    target = jnp.broadcast_to(live, system.shape[:-1])
    beta = solve_small(system, target)
    return beta / lax.optimization_barrier(jnp.sum(beta, axis=-1, keepdims=True))

def block_out(operands):
    values, gate_w, up_w, down_w, gain_row = operands
    normed = rms_scaled(values, gain_row)
    gate_val = jnp.dot(normed, gate_w, preferred_element_type=jnp.float32)
    up_val = jnp.dot(normed, up_w, preferred_element_type=jnp.float32)
    hidden = (jax.nn.silu(gate_val) * up_val).astype(jnp.bfloat16)
    grouped = hidden.reshape(TOKENS, N_DP, FF // N_DP).transpose(1, 0, 2).astype(jnp.float32)
    down_groups = down_w.reshape(N_DP, FF // N_DP, D).astype(jnp.float32)
    partials = jnp.einsum('gtf,gfd->gtd', grouped, down_groups).astype(jnp.bfloat16).astype(jnp.float32)
    total = lax.optimization_barrier(jnp.sum(partials, axis=0))
    return (values + total).astype(jnp.bfloat16)

def reference(inject, w_gate, w_up, w_down, gain):
    source = inject.astype(jnp.float32)
    iterate = jnp.zeros((SECTIONS, TOKENS, D), jnp.float32)
    images = jnp.zeros((HIST, SECTIONS, TOKENS, D), jnp.float32)
    misfits = jnp.zeros((HIST, SECTIONS, TOKENS, D), jnp.float32)
    mixing = jnp.zeros((SECTIONS, ITERS, HIST), jnp.float32)
    cell_count = float(TOKENS * D)
    for iteration in range(ITERS):
        output = lax.map(block_out, (iterate, w_gate, w_up, w_down, gain))
        mapped = source + 0.5 * jnp.roll(output, 1, axis=0).astype(jnp.float32)
        misfit = mapped - iterate
        images = images.at[iteration].set(mapped)
        misfits = misfits.at[iteration].set(misfit)
        gram_matrix = jnp.einsum('hstd,gstd->shg', misfits, misfits, precision=lax.Precision.HIGHEST) / cell_count
        weights = mixing_weights(gram_matrix, iteration)
        mixing = mixing.at[:, iteration].set(weights)
        iterate = jnp.einsum('sh,hstd->std', weights, images, precision=lax.Precision.HIGHEST)
    return (iterate, mixing)
```

```python
import jax
import jax.numpy as jnp
from jax import lax
from jax.experimental import pallas as pl
from jax.experimental.pallas import tpu as pltpu
from jax.sharding import PartitionSpec as P

ITERS = 5
HIST = 5
SECTIONS = 8
RING = 4
N_DP = 32
ROWS = 8
PACK = RING * ROWS
TOK = RING * PACK
D = 4096
FFL = 344
FFP = 384
CHUNKS = 4
CH = D // CHUNKS
NT = 512
MESH = pl.DeviceIdType.MESH
F32 = jnp.float32
BF16 = jnp.bfloat16


def solve_small(entries, values):
    count = len(values)
    entries = [list(row) for row in entries]
    values = list(values)
    for p in range(count):
        for i in range(p + 1, count):
            factor = entries[i][p] / entries[p][p]
            for j in range(p, count):
                entries[i][j] = entries[i][j] - factor * entries[p][j]
            values[i] = values[i] - factor * values[p]
    answer = [None] * count
    for i in range(count - 1, -1, -1):
        accum = values[i]
        for j in range(i + 1, count):
            accum = accum - entries[i][j] * answer[j]
        answer[i] = accum / entries[i][i]
    return answer


def kernel(
    inject_ref, gain_ref, wg_hbm, wu_hbm, wd_hbm,
    iterate_ref, mixing_ref,
    wgu, wd, acc, hid, images, misfits, x_ref,
    nsend, nrecv, g, p, pr, q, qown, qr, osend, orecv, gmsg, grecv, gram_s,
    w_local, w_send, w_recv,
    as_send, as_recv, ab_send, ab_recv, rb_send, rb_recv, rs_send, rs_recv,
    z_send, z_recv, g_send, g_recv,
):
    sec = lax.axis_index("section")
    dp = lax.axis_index("dp")
    core = lax.rem(dp, 2)
    cx = lax.div(dp, 8)
    cy = lax.rem(lax.div(dp, 2), RING)
    small = cx + core * (cy - cx)
    big = cy + core * (cx - cy)
    step_small = 8 - 6 * core
    step_big = 2 + 6 * core

    def at_small(j):
        return (sec, lax.rem(small + RING + j, RING) * step_small + big * step_big + core)

    def at_big(j):
        return (sec, small * step_small + lax.rem(big + RING + j, RING) * step_big + core)

    sibling = (sec, dp + 1 - 2 * core)
    after = (lax.rem(sec + 1, SECTIONS), dp)
    before = (lax.rem(sec + SECTIONS - 1, SECTIONS), dp)

    def remote(src, dst, send, recv, device):
        return pltpu.make_async_remote_copy(
            src_ref=src, dst_ref=dst, send_sem=send, recv_sem=recv, device_id=device, device_id_type=MESH
        )

    local_copies = [
        pltpu.make_async_copy(wg_hbm, wgu.at[pl.ds(0, FFL), :], w_local.at[0]),
        pltpu.make_async_copy(wu_hbm, wgu.at[pl.ds(2 * FFP, FFL), :], w_local.at[1]),
        pltpu.make_async_copy(wd_hbm, wd.at[pl.ds(0, FFL), :], w_local.at[2]),
    ]
    shared_copies = [
        remote(wg_hbm, wgu.at[pl.ds(FFP, FFL), :], w_send.at[0], w_recv.at[0], sibling),
        remote(wu_hbm, wgu.at[pl.ds(3 * FFP, FFL), :], w_send.at[1], w_recv.at[1], sibling),
        remote(wd_hbm, wd.at[pl.ds(FFP, FFL), :], w_send.at[2], w_recv.at[2], sibling),
    ]
    for copy in local_copies:
        copy.start()

    barrier = pltpu.get_barrier_semaphore()

    @pl.loop(1, N_DP)
    def _(d):
        pl.semaphore_signal(barrier, inc=1, device_id=(sec, lax.rem(dp + d, N_DP)), device_id_type=MESH)

    pl.semaphore_signal(barrier, inc=1, device_id=after, device_id_type=MESH)
    pl.semaphore_signal(barrier, inc=1, device_id=before, device_id_type=MESH)

    x_ref[...] = jnp.zeros_like(x_ref)
    images[...] = jnp.zeros_like(images)
    misfits[...] = jnp.zeros_like(misfits)
    gram_s[...] = jnp.zeros_like(gram_s)
    for h in range(2):
        wd[h * FFP + FFL : (h + 1) * FFP, :] = jnp.zeros((FFP - FFL, D), BF16)

    pl.semaphore_wait(barrier, N_DP + 1)
    for copy in shared_copies:
        copy.start()

    lane = lax.broadcasted_iota(jnp.int32, (1, 128), 1)
    cells = float(ROWS * N_DP * D)

    def cols(c):
        return pl.ds(c * CH, CH)

    def small_gather(c, j):
        return remote(
            nsend.at[:, cols(c)], nrecv.at[j - 1, :, cols(c)], as_send.at[c, j - 1], as_recv.at[c, j - 1], at_small(j)
        )

    def big_gather(c, j):
        return remote(
            g.at[0, :, cols(c)], g.at[j, :, cols(c)], ab_send.at[c, j - 1], ab_recv.at[c, j - 1], at_big(j)
        )

    def big_reduce(c, j):
        return remote(
            p.at[j, :, cols(c)], pr.at[j - 1, :, cols(c)], rb_send.at[c, j - 1], rb_recv.at[c, j - 1], at_big(-j)
        )

    def small_reduce(c, j):
        return remote(
            q.at[j - 1, :, cols(c)], qr.at[j - 1, :, cols(c)], rs_send.at[c, j - 1], rs_recv.at[c, j - 1], at_small(-j)
        )

    @pl.loop(0, ITERS)
    def _(k):
        parity = lax.rem(k, 2)

        def relay(c):
            return remote(
                osend.at[:, cols(c)], orecv.at[k, :, cols(c)], z_send.at[c], z_recv.at[k, c], after
            )

        x = x_ref[...]
        inverse = lax.rsqrt(jnp.mean(x * x, axis=-1, keepdims=True) + 1e-06)
        for c in range(CHUNKS):
            nsend[:, cols(c)] = (x_ref[:, cols(c)] * inverse * gain_ref[:, cols(c)]).astype(BF16)

        @pl.when(k > 0)
        def _():
            for c in range(CHUNKS):
                for j in (1, 3, 2):
                    small_gather(c, j).start()
            for c in range(CHUNKS):
                for j in (1, 3, 2):
                    small_gather(c, j).wait_recv()
                rows = [nsend[:, cols(c)].astype(F32)] + [nrecv[j, :, cols(c)].astype(F32) for j in range(3)]
                g[0, :, cols(c)] = jnp.concatenate(rows, axis=0).astype(BF16)
                for j in (1, 3, 2):
                    big_gather(c, j).start()

        @pl.when(k == 0)
        def _():
            for c in range(CHUNKS):
                mine = nsend[:, cols(c)].astype(F32)
                packed = jnp.concatenate([mine] * RING, axis=0).astype(BF16)
                for j in range(RING):
                    g[j, :, cols(c)] = packed
            for copy in local_copies:
                copy.wait()
            for copy in shared_copies:
                copy.wait_recv()

        for c in range(CHUNKS):
            @pl.when(k > 0)
            def _():
                for j in (1, 3, 2):
                    big_gather(c, j).wait_recv()

            tokens = g[:, :, cols(c)].reshape(TOK, CH)

            @pl.loop(0, 4 * FFP // NT)
            def _(n):
                at = pl.ds(pl.multiple_of(n * NT, NT), NT)
                product = lax.dot_general(
                    tokens, wgu[at, cols(c)], (((1,), (1,)), ((), ())), preferred_element_type=F32
                )
                if c == 0:
                    acc[:, at] = product
                else:
                    acc[:, at] += product

        for h in range(2):
            gate = acc[:, h * FFP : (h + 1) * FFP]
            up = acc[:, (2 + h) * FFP : (3 + h) * FFP]
            value = gate / (1.0 + jnp.exp(-gate)) * up
            real = lax.broadcasted_iota(jnp.int32, (TOK, FFP), 1) < FFL
            hid[:, h * FFP : (h + 1) * FFP] = jnp.where(real, value, 0.0).astype(BF16)

        for c in range(CHUNKS):
            product = jnp.dot(hid[...], wd[:, cols(c)], preferred_element_type=F32).astype(BF16)
            p[:, :, cols(c)] = product.reshape(RING, PACK, CH)
            for j in (1, 3, 2):
                big_reduce(c, j).start()

        for c in range(CHUNKS):
            for j in (1, 3, 2):
                big_reduce(c, j).wait_recv()
            total = p[0, :, cols(c)].astype(F32)
            for j in range(3):
                total = total + pr[j, :, cols(c)].astype(F32)
            qown[:, cols(c)] = total[:ROWS]
            for j in (1, 3, 2):
                q[j - 1, :, cols(c)] = total[j * ROWS : (j + 1) * ROWS].astype(BF16)
                small_reduce(c, j).start()

        for c in range(CHUNKS):
            for j in (1, 3, 2):
                small_reduce(c, j).wait_recv()
            total = qown[:, cols(c)]
            for j in range(3):
                total = total + qr[j, :, cols(c)].astype(F32)
            osend[:, cols(c)] = (x_ref[:, cols(c)] + total).astype(BF16)
            relay(c).start()

        sums = [jnp.zeros((ROWS, CH), F32) for _ in range(HIST)]
        for c in range(CHUNKS):
            relay(c).wait_recv()
            mapped = inject_ref[:, cols(c)].astype(F32) + 0.5 * orecv[k, :, cols(c)].astype(F32)
            misfit = mapped - x_ref[:, cols(c)]
            images[k, :, cols(c)] = mapped
            misfits[k, :, cols(c)] = misfit
            sums = [sums[i] + misfit * misfits[i, :, cols(c)] for i in range(HIST)]
        row = jnp.zeros((1, 128), F32)
        for i in range(HIST):
            value = jnp.sum(jnp.sum(sums[i], axis=0, keepdims=True), axis=1, keepdims=True)
            row = jnp.where(lane == i, value, row)
        gmsg[...] = row

        @pl.loop(1, N_DP)
        def _(d):
            remote(
                gmsg, grecv.at[parity, d - 1], g_send, g_recv.at[parity], (sec, lax.rem(dp + d, N_DP))
            ).start()

        @pl.when(k > 0)
        def _():
            for c in range(CHUNKS):
                for j in (1, 3, 2):
                    small_gather(c, j).wait_send()
                    big_gather(c, j).wait_send()
        for c in range(CHUNKS):
            for j in (1, 3, 2):
                big_reduce(c, j).wait_send()
                small_reduce(c, j).wait_send()
            relay(c).wait_send()
        pltpu.make_async_copy(grecv.at[parity], grecv.at[parity], g_recv.at[parity]).wait()
        row = (row + jnp.sum(grecv[parity], axis=0)) / cells
        pltpu.make_async_copy(grecv.at[parity], grecv.at[parity], g_send).wait()

        fresh = [
            jnp.broadcast_to(jnp.sum(jnp.where(lane == i, row, 0.0), axis=1, keepdims=True), (8, 128))
            for i in range(HIST)
        ]
        gram = [[None] * HIST for _ in range(HIST)]
        for i in range(HIST):
            for j in range(i + 1):
                slot = i * (i + 1) // 2 + j
                entry = jnp.where(k == i, fresh[j], gram_s[slot])
                gram_s[slot] = entry
                gram[i][j] = entry
                gram[j][i] = entry
        steps = jnp.full((8, 128), k + 1, jnp.int32)
        live = [jnp.where(steps > i, 1.0, 0.0) for i in range(HIST)]
        trace = gram[0][0]
        for i in range(1, HIST):
            trace = trace + gram[i][i]
        damp = 0.01 * trace / steps.astype(F32) + 1e-06
        system = [[gram[i][j] * live[i] * live[j] for j in range(HIST)] for i in range(HIST)]
        for i in range(HIST):
            system[i][i] = system[i][i] + (live[i] * damp + (1.0 - live[i]))
        beta = solve_small(system, live)
        whole = beta[0]
        for i in range(1, HIST):
            whole = whole + beta[i]
        weights = [value / whole for value in beta]
        mixed = jnp.zeros((1, 128), F32)
        for i in range(HIST):
            mixed = jnp.where(lane == i, weights[i][:1], mixed)
        mixing_ref[pl.ds(k, 1), :] = mixed[:, :HIST]
        for c in range(D // 128):
            at = pl.ds(c * 128, 128)
            value = weights[0] * images[0, :, at]
            for i in range(1, HIST):
                value = value + weights[i] * images[i, :, at]
            x_ref[:, at] = value

    for copy in shared_copies:
        copy.wait_send()
    iterate_ref[...] = x_ref[...]


def local(inject, w_gate, w_up, w_down, gain):
    vmem = pl.BlockSpec(memory_space=pltpu.VMEM)
    hbm = pl.BlockSpec(memory_space=pl.ANY)
    dma = pltpu.SemaphoreType.DMA
    iterate, mixing = pl.pallas_call(
        kernel,
        out_shape=(jax.ShapeDtypeStruct((ROWS, D), F32), jax.ShapeDtypeStruct((ITERS, HIST), F32)),
        in_specs=[vmem, vmem, hbm, hbm, hbm],
        out_specs=(vmem, vmem),
        scratch_shapes=[
            pltpu.VMEM((4 * FFP, D), BF16),
            pltpu.VMEM((2 * FFP, D), BF16),
            pltpu.VMEM((TOK, 4 * FFP), F32),
            pltpu.VMEM((TOK, 2 * FFP), BF16),
            pltpu.VMEM((HIST, ROWS, D), F32),
            pltpu.VMEM((HIST, ROWS, D), F32),
            pltpu.VMEM((ROWS, D), F32),
            pltpu.VMEM((ROWS, D), BF16),
            pltpu.VMEM((3, ROWS, D), BF16),
            pltpu.VMEM((RING, PACK, D), BF16),
            pltpu.VMEM((RING, PACK, D), BF16),
            pltpu.VMEM((3, PACK, D), BF16),
            pltpu.VMEM((3, ROWS, D), BF16),
            pltpu.VMEM((ROWS, D), F32),
            pltpu.VMEM((3, ROWS, D), BF16),
            pltpu.VMEM((ROWS, D), BF16),
            pltpu.VMEM((ITERS, ROWS, D), BF16),
            pltpu.VMEM((1, 128), F32),
            pltpu.VMEM((2, N_DP - 1, 1, 128), F32),
            pltpu.VMEM((HIST * (HIST + 1) // 2, 8, 128), F32),
            dma((3,)), dma((3,)), dma((3,)),
            dma((CHUNKS, 3)), dma((CHUNKS, 3)), dma((CHUNKS, 3)), dma((CHUNKS, 3)),
            dma((CHUNKS, 3)), dma((CHUNKS, 3)), dma((CHUNKS, 3)), dma((CHUNKS, 3)),
            dma((CHUNKS,)), dma((ITERS, CHUNKS)), dma, dma((2,)),
        ],
        compiler_params=pltpu.CompilerParams(
            collective_id=0, has_side_effects=True, vmem_limit_bytes=62 * 1024 * 1024
        ),
    )(inject[0], gain, w_gate[0].T, w_up[0].T, w_down[0])
    return iterate[None], mixing[None]


def solution(mesh):
    return jax.shard_map(
        local,
        mesh=mesh,
        in_specs=(
            P("section", "dp", None),
            P("section", None, "dp"),
            P("section", None, "dp"),
            P("section", "dp", None),
            P("section", None),
        ),
        out_specs=(P("section", "dp", None), P("section", None, None)),
        check_vma=False,
    )
```

```python
import jax
import jax.numpy as jnp
from jax import lax
from jax.experimental import pallas as pl
from jax.experimental.pallas import tpu as pltpu
from jax.sharding import PartitionSpec as P

ITERS = 5
HIST = 5
SECTIONS = 8
RING = 4
N_DP = 32
ROWS = 8
PACK = RING * ROWS
TOK = RING * PACK
D = 4096
FFL = 344
FFP = 384
CHUNKS = 4
CH = D // CHUNKS
NT = 512
RELAYED = ()
HALF = PACK // 2
LOW = pl.ds(0, HALF)
HIGH = pl.ds(HALF, HALF)
MESH = pl.DeviceIdType.MESH
F32 = jnp.float32
BF16 = jnp.bfloat16


def solve_small(entries, values):
    count = len(values)
    entries = [list(row) for row in entries]
    values = list(values)
    for p in range(count):
        for i in range(p + 1, count):
            factor = entries[i][p] / entries[p][p]
            for j in range(p, count):
                entries[i][j] = entries[i][j] - factor * entries[p][j]
            values[i] = values[i] - factor * values[p]
    answer = [None] * count
    for i in range(count - 1, -1, -1):
        accum = values[i]
        for j in range(i + 1, count):
            accum = accum - entries[i][j] * answer[j]
        answer[i] = accum / entries[i][i]
    return answer


def kernel(
    inject_ref, gain_ref, wg_hbm, wu_hbm, wd_hbm,
    iterate_ref, mixing_ref,
    wgu, wgt, eye, wd, pre, hid, images, misfits, x_ref, prev,
    nsend, nrecv, g, p, ph, pr, q, qown, qr, osend, orecv, gmsg, grecv, gram_s, coef, inv_s, inv_w,
    w_local, w_send, w_recv,
    as_send, as_recv, ab_send, ab_recv, rb_send, rb_recv, rs_send, rs_recv,
    z_send, z_recv, g_send, g_recv, i_send, i_recv,
):
    sec = lax.axis_index("section")
    dp = lax.axis_index("dp")
    core = lax.rem(dp, 2)
    cx = lax.div(dp, 8)
    cy = lax.rem(lax.div(dp, 2), RING)
    small = cx + core * (cy - cx)
    big = cy + core * (cx - cy)
    step_small = 8 - 6 * core
    step_big = 2 + 6 * core

    def at_small(j):
        return (sec, lax.rem(small + RING + j, RING) * step_small + big * step_big + core)

    def at_big(j):
        return (sec, small * step_small + lax.rem(big + RING + j, RING) * step_big + core)

    sibling = (sec, dp + 1 - 2 * core)
    after = (lax.rem(sec + 1, SECTIONS), dp)
    before = (lax.rem(sec + SECTIONS - 1, SECTIONS), dp)

    def remote(src, dst, send, recv, device):
        return pltpu.make_async_remote_copy(
            src_ref=src, dst_ref=dst, send_sem=send, recv_sem=recv, device_id=device, device_id_type=MESH
        )

    local_copies = [
        pltpu.make_async_copy(wg_hbm, wgu.at[pl.ds(0, FFL), :], w_local.at[0]),
        pltpu.make_async_copy(wu_hbm, wgu.at[pl.ds(FFP, FFL), :], w_local.at[1]),
    ]
    shared_copies = [
        remote(wg_hbm, wgu.at[pl.ds(2 * FFP, FFL), :], w_send.at[0], w_recv.at[0], sibling),
        remote(wu_hbm, wgu.at[pl.ds(3 * FFP, FFL), :], w_send.at[1], w_recv.at[1], sibling),
    ]
    for c in range(CHUNKS):
        at = pl.ds(c * CH, CH)
        local_copies.append(pltpu.make_async_copy(wd_hbm.at[:, at], wd.at[pl.ds(0, FFL), at], w_local.at[2 + c]))
        shared_copies.append(
            remote(wd_hbm.at[:, at], wd.at[pl.ds(FFP, FFL), at], w_send.at[2 + c], w_recv.at[2 + c], sibling)
        )
    local_copies = local_copies[2:] + local_copies[:2]
    shared_copies = shared_copies[2:] + shared_copies[:2]
    for copy in local_copies:
        copy.start()

    barrier = pltpu.get_barrier_semaphore()

    @pl.loop(1, N_DP)
    def _(d):
        pl.semaphore_signal(barrier, inc=1, device_id=(sec, lax.rem(dp + d, N_DP)), device_id_type=MESH)

    pl.semaphore_signal(barrier, inc=1, device_id=after, device_id_type=MESH)
    pl.semaphore_signal(barrier, inc=1, device_id=before, device_id_type=MESH)

    for ref in (x_ref, prev, images, misfits, gram_s, coef):
        ref[...] = jnp.zeros_like(ref)
    for l in range(HIST - 1):
        pre[l] = jnp.zeros((TOK, 4 * FFP), F32)
    for h in range(2):
        wgu[2 * h * FFP + FFL : (2 * h + 1) * FFP, :] = jnp.zeros((FFP - FFL, D), BF16)
        wgu[(2 * h + 1) * FFP + FFL : (2 * h + 2) * FFP, :] = jnp.zeros((FFP - FFL, D), BF16)
        wd[h * FFP + FFL : (h + 1) * FFP, :] = jnp.zeros((FFP - FFL, D), BF16)

    corner = lax.broadcasted_iota(jnp.int32, (256, 256), 0) == lax.broadcasted_iota(jnp.int32, (256, 256), 1)
    eye[...] = jnp.where(corner, 1.0, 0.0).astype(BF16)

    def turn(half):
        @pl.loop(0, D // 256)
        def _(n):
            at = pl.ds(pl.multiple_of(n * 256, 256), 256)
            rows = pl.ds(half * 2 * FFP, 2 * FFP)
            wgt[at, rows] = lax.dot_general(
                eye[...], wgu[rows, at], (((1,), (1,)), ((), ())), preferred_element_type=F32
            ).astype(BF16)

    pl.semaphore_wait(barrier, N_DP + 1)
    for copy in shared_copies:
        copy.start()

    lane = lax.broadcasted_iota(jnp.int32, (1, 128), 1)
    wide = lax.broadcasted_iota(jnp.int32, (ROWS, 128), 1)
    first = jnp.where(wide < ROWS, 1.0, 0.0)
    diagonal = lax.rem(wide, ROWS) == lax.broadcasted_iota(jnp.int32, (ROWS, 128), 0)
    cells = float(ROWS * N_DP * D)

    def cols(c):
        return pl.ds(c * CH, CH)

    def small_gather(c, j):
        return remote(
            nsend.at[:, cols(c)], nrecv.at[j - 1, :, cols(c)], as_send.at[c, j - 1], as_recv.at[c, j - 1], at_small(j)
        )

    def big_gather(c, i):
        src, dst, at = (
            (g.at[0, :, cols(c)], g.at[1, :, cols(c)], 1),
            (g.at[0, :, cols(c)], g.at[3, :, cols(c)], -1),
            (g.at[1, LOW, cols(c)], g.at[2, LOW, cols(c)], 1),
            (g.at[3, HIGH, cols(c)], g.at[2, HIGH, cols(c)], -1),
            (g.at[0, :, cols(c)], g.at[2, :, cols(c)], 2),
        )[i]
        return remote(src, dst, ab_send.at[c, i], ab_recv.at[c, i], at_big(at))

    def big_reduce(c, i):
        src, dst, at = (
            (p.at[2, LOW, cols(c)], ph.at[0, :, cols(c)], 1),
            (p.at[2, HIGH, cols(c)], ph.at[1, :, cols(c)], -1),
            (p.at[3, HIGH, cols(c)], pr.at[0, HIGH, cols(c)], 1),
            (p.at[1, LOW, cols(c)], pr.at[1, LOW, cols(c)], -1),
            (p.at[3, LOW, cols(c)], pr.at[0, LOW, cols(c)], 1),
            (p.at[1, HIGH, cols(c)], pr.at[1, HIGH, cols(c)], -1),
            (p.at[2, :, cols(c)], pr.at[2, :, cols(c)], 2),
            (p.at[3, :, cols(c)], pr.at[0, :, cols(c)], 1),
            (p.at[1, :, cols(c)], pr.at[1, :, cols(c)], -1),
        )[i]
        return remote(src, dst, rb_send.at[c, i], rb_recv.at[c, i], at_big(at))

    def small_reduce(c, j):
        return remote(
            q.at[j - 1, :, cols(c)], qr.at[j - 1, :, cols(c)], rs_send.at[c, j - 1], rs_recv.at[c, j - 1], at_small(-j)
        )

    @pl.loop(0, ITERS)
    def _(k):
        parity = lax.rem(k, 2)

        def relay(c):
            return remote(
                osend.at[:, cols(c)], orecv.at[k, :, cols(c)], z_send.at[c], z_recv.at[k, c], after
            )

        def own_inverse():
            x = x_ref[...]
            return lax.rsqrt(jnp.mean(x * x, axis=-1, keepdims=True) + 1e-06)

        def tell_inverse(slot):
            i, j = lax.rem(slot, RING), lax.div(slot, RING)
            at = lax.rem(small + i, RING) * step_small + lax.rem(big + j, RING) * step_big + core
            return remote(inv_s.at[0], inv_s.at[slot], i_send, i_recv, (sec, at))

        others = inv_s.at[pl.ds(1, RING * RING - 1)]

        @pl.when(k == 0)
        def _():
            spread = jnp.sum(jnp.where(diagonal, own_inverse(), 0.0), axis=0, keepdims=True)
            for slot in range(RING * RING):
                inv_s[slot] = spread

        @pl.when(k > 0)
        def _():
            pltpu.make_async_copy(others, others, i_recv).wait()
            pltpu.make_async_copy(others, others, i_send).wait()

        for slot in range(RING * RING):
            column = jnp.sum(jnp.where(diagonal, inv_s[slot], 0.0) * first, axis=1, keepdims=True)
            inv_w[slot * ROWS : (slot + 1) * ROWS, :] = jnp.broadcast_to(column, (ROWS, 128))
        inverse = inv_w[...]

        def product_of(at):
            value = coef[0, :1] * pre[0, :, at]
            for l in range(1, HIST - 1):
                value = value + coef[l, :1] * pre[l, :, at]
            return value * inverse

        for h in range(2):
            for t in range(FFP // 128):
                gate = product_of(pl.ds(2 * h * FFP + t * 128, 128))
                up = product_of(pl.ds((2 * h + 1) * FFP + t * 128, 128))
                value = gate / (1.0 + jnp.exp(-gate)) * up
                real = lax.broadcasted_iota(jnp.int32, (TOK, 128), 1) < FFL - t * 128
                hid[:, h * FFP + t * 128 : h * FFP + (t + 1) * 128] = jnp.where(real, value, 0.0).astype(BF16)

        for c in range(CHUNKS):
            @pl.when(k == 0)
            def _():
                local_copies[c].wait()
                shared_copies[c].wait_recv()

            product = jnp.dot(hid[...], wd[:, cols(c)], preferred_element_type=F32).astype(BF16)
            p[:, :, cols(c)] = product.reshape(RING, PACK, CH)
            for i in (0, 1, 2, 3) if c in RELAYED else (6, 7, 8):
                big_reduce(c, i).start()

        @pl.when(k == 0)
        def _():
            for copy in local_copies[CHUNKS:]:
                copy.wait()
            turn(0)

        for c in RELAYED:
            big_reduce(c, 0).wait_recv()
            p[3, LOW, cols(c)] = (p[3, LOW, cols(c)].astype(F32) + ph[0, :, cols(c)].astype(F32)).astype(BF16)
            big_reduce(c, 4).start()
            big_reduce(c, 1).wait_recv()
            p[1, HIGH, cols(c)] = (p[1, HIGH, cols(c)].astype(F32) + ph[1, :, cols(c)].astype(F32)).astype(BF16)
            big_reduce(c, 5).start()

        for c in range(CHUNKS):
            for i in (2, 3, 4, 5) if c in RELAYED else (6, 7, 8):
                big_reduce(c, i).wait_recv()
            total = p[0, :, cols(c)].astype(F32)
            for j in range(2 if c in RELAYED else 3):
                total = total + pr[j, :, cols(c)].astype(F32)
            qown[:, cols(c)] = total[:ROWS]
            for j in (1, 3, 2):
                q[j - 1, :, cols(c)] = total[j * ROWS : (j + 1) * ROWS].astype(BF16)
                small_reduce(c, j).start()

        for c in range(CHUNKS):
            for j in (1, 3, 2):
                small_reduce(c, j).wait_recv()
            total = qown[:, cols(c)]
            for j in range(3):
                total = total + qr[j, :, cols(c)].astype(F32)
            osend[:, cols(c)] = (x_ref[:, cols(c)] + total).astype(BF16)
            relay(c).start()

        sums = [jnp.zeros((ROWS, CH), F32) for _ in range(HIST)]
        for c in range(CHUNKS):
            relay(c).wait_recv()
            mapped = inject_ref[:, cols(c)].astype(F32) + 0.5 * orecv[k, :, cols(c)].astype(F32)
            misfit = mapped - x_ref[:, cols(c)]
            images[k, :, cols(c)] = mapped
            misfits[k, :, cols(c)] = misfit
            nsend[:, cols(c)] = ((mapped - prev[:, cols(c)]) * gain_ref[:, cols(c)]).astype(BF16)
            prev[:, cols(c)] = mapped

            @pl.when(k < ITERS - 1)
            def _():
                for j in (1, 3, 2):
                    small_gather(c, j).start()

            sums = [sums[i] + misfit * misfits[i, :, cols(c)] for i in range(HIST)]
        row = jnp.zeros((1, 128), F32)
        for i in range(HIST):
            value = jnp.sum(jnp.sum(sums[i], axis=0, keepdims=True), axis=1, keepdims=True)
            row = jnp.where(lane == i, value, row)
        gmsg[...] = row

        @pl.loop(1, N_DP)
        def _(d):
            remote(
                gmsg, grecv.at[parity, d - 1], g_send, g_recv.at[parity], (sec, lax.rem(dp + d, N_DP))
            ).start()

        for c in range(CHUNKS):
            for i in range(6) if c in RELAYED else (6, 7, 8):
                big_reduce(c, i).wait_send()
            for j in (1, 3, 2):
                small_reduce(c, j).wait_send()
            relay(c).wait_send()

        @pl.when(k < ITERS - 1)
        def _():
            @pl.when(k == 0)
            def _():
                for copy in shared_copies[CHUNKS:]:
                    copy.wait_recv()
                turn(1)

            for c in range(CHUNKS):
                for j in (1, 3, 2):
                    small_gather(c, j).wait_recv()
                rows = [nsend[:, cols(c)].astype(F32)] + [nrecv[j, :, cols(c)].astype(F32) for j in range(3)]
                g[0, :, cols(c)] = jnp.concatenate(rows, axis=0).astype(BF16)
                for i in (0, 1) if c in RELAYED else (4, 0, 1):
                    big_gather(c, i).start()

            for c in RELAYED:
                big_gather(c, 0).wait_recv()
                big_gather(c, 2).start()
                big_gather(c, 1).wait_recv()
                big_gather(c, 3).start()

        pltpu.make_async_copy(grecv.at[parity], grecv.at[parity], g_recv.at[parity]).wait()
        row = (row + jnp.sum(grecv[parity], axis=0)) / cells
        pltpu.make_async_copy(grecv.at[parity], grecv.at[parity], g_send).wait()

        fresh = [
            jnp.broadcast_to(jnp.sum(jnp.where(lane == i, row, 0.0), axis=1, keepdims=True), (8, 128))
            for i in range(HIST)
        ]
        gram = [[None] * HIST for _ in range(HIST)]
        for i in range(HIST):
            for j in range(i + 1):
                slot = i * (i + 1) // 2 + j
                entry = jnp.where(k == i, fresh[j], gram_s[slot])
                gram_s[slot] = entry
                gram[i][j] = entry
                gram[j][i] = entry
        steps = jnp.full((8, 128), k + 1, jnp.int32)
        live = [jnp.where(steps > i, 1.0, 0.0) for i in range(HIST)]
        trace = gram[0][0]
        for i in range(1, HIST):
            trace = trace + gram[i][i]
        damp = 0.01 * trace / steps.astype(F32) + 1e-06
        system = [[gram[i][j] * live[i] * live[j] for j in range(HIST)] for i in range(HIST)]
        for i in range(HIST):
            system[i][i] = system[i][i] + (live[i] * damp + (1.0 - live[i]))
        beta = solve_small(system, live)
        whole = beta[0]
        for i in range(1, HIST):
            whole = whole + beta[i]
        weights = [value / whole for value in beta]
        mixed = jnp.zeros((1, 128), F32)
        for i in range(HIST):
            mixed = jnp.where(lane == i, weights[i][:1], mixed)
        mixing_ref[pl.ds(k, 1), :] = mixed[:, :HIST]
        for l in range(HIST - 1):
            tail = weights[l]
            for i in range(l + 1, HIST):
                tail = tail + weights[i]
            coef[l] = tail
        for c in range(D // 128):
            at = pl.ds(c * 128, 128)
            value = weights[0] * images[0, :, at]
            for i in range(1, HIST):
                value = value + weights[i] * images[i, :, at]
            x_ref[:, at] = value

        @pl.when(k < ITERS - 1)
        def _():
            inv_s[0] = jnp.sum(jnp.where(diagonal, own_inverse(), 0.0), axis=0, keepdims=True)

            @pl.loop(1, RING * RING)
            def _(slot):
                tell_inverse(slot).start()

            for c in range(CHUNKS):
                for i in (2, 3) if c in RELAYED else (0, 1, 4):
                    big_gather(c, i).wait_recv()
                tokens = g[:, :, cols(c)].reshape(TOK, CH)

                @pl.loop(0, 4 * FFP // NT)
                def _(n):
                    at = pl.ds(pl.multiple_of(n * NT, NT), NT)
                    product = jnp.dot(tokens, wgt[cols(c), at], preferred_element_type=F32)
                    if c == 0:
                        pre[k, :, at] = product
                    else:
                        pre[k, :, at] += product

            for c in range(CHUNKS):
                for j in (1, 3, 2):
                    small_gather(c, j).wait_send()
                for i in range(4) if c in RELAYED else (0, 1, 4):
                    big_gather(c, i).wait_send()

    for copy in shared_copies:
        copy.wait_send()
    iterate_ref[...] = x_ref[...]


def local(inject, w_gate, w_up, w_down, gain):
    vmem = pl.BlockSpec(memory_space=pltpu.VMEM)
    hbm = pl.BlockSpec(memory_space=pl.ANY)
    dma = pltpu.SemaphoreType.DMA
    iterate, mixing = pl.pallas_call(
        kernel,
        out_shape=(jax.ShapeDtypeStruct((ROWS, D), F32), jax.ShapeDtypeStruct((ITERS, HIST), F32)),
        in_specs=[vmem, vmem, hbm, hbm, hbm],
        out_specs=(vmem, vmem),
        scratch_shapes=[
            pltpu.VMEM((4 * FFP, D), BF16),
            pltpu.VMEM((D, 4 * FFP), BF16),
            pltpu.VMEM((256, 256), BF16),
            pltpu.VMEM((2 * FFP, D), BF16),
            pltpu.VMEM((HIST - 1, TOK, 4 * FFP), F32),
            pltpu.VMEM((TOK, 2 * FFP), BF16),
            pltpu.VMEM((HIST, ROWS, D), F32),
            pltpu.VMEM((HIST, ROWS, D), F32),
            pltpu.VMEM((ROWS, D), F32),
            pltpu.VMEM((ROWS, D), F32),
            pltpu.VMEM((ROWS, D), BF16),
            pltpu.VMEM((3, ROWS, D), BF16),
            pltpu.VMEM((RING, PACK, D), BF16),
            pltpu.VMEM((RING, PACK, D), BF16),
            pltpu.VMEM((2, HALF, D), BF16),
            pltpu.VMEM((3, PACK, D), BF16),
            pltpu.VMEM((3, ROWS, D), BF16),
            pltpu.VMEM((ROWS, D), F32),
            pltpu.VMEM((3, ROWS, D), BF16),
            pltpu.VMEM((ROWS, D), BF16),
            pltpu.VMEM((ITERS, ROWS, D), BF16),
            pltpu.VMEM((1, 128), F32),
            pltpu.VMEM((2, N_DP - 1, 1, 128), F32),
            pltpu.VMEM((HIST * (HIST + 1) // 2, 8, 128), F32),
            pltpu.VMEM((HIST - 1, 8, 128), F32),
            pltpu.VMEM((RING * RING, 1, 128), F32),
            pltpu.VMEM((TOK, 128), F32),
            dma((2 + CHUNKS,)), dma((2 + CHUNKS,)), dma((2 + CHUNKS,)),
            dma((CHUNKS, 3)), dma((CHUNKS, 3)), dma((CHUNKS, 5)), dma((CHUNKS, 5)),
            dma((CHUNKS, 9)), dma((CHUNKS, 9)), dma((CHUNKS, 3)), dma((CHUNKS, 3)),
            dma((CHUNKS,)), dma((ITERS, CHUNKS)), dma, dma((2,)), dma, dma,
        ],
        compiler_params=pltpu.CompilerParams(
            collective_id=0, has_side_effects=True, vmem_limit_bytes=62 * 1024 * 1024
        ),
    )(inject[0], gain, w_gate[0].T, w_up[0].T, w_down[0])
    return iterate[None], mixing[None]


def solution(mesh):
    return jax.shard_map(
        local,
        mesh=mesh,
        in_specs=(
            P("section", "dp", None),
            P("section", None, "dp"),
            P("section", None, "dp"),
            P("section", "dp", None),
            P("section", None),
        ),
        out_specs=(P("section", "dp", None), P("section", None, None)),
        check_vma=False,
    )
```

```python
import jax
import jax.numpy as jnp
from jax import lax
from jax.experimental import pallas as pl
from jax.experimental.pallas import tpu as pltpu
from jax.sharding import PartitionSpec as P

ITERS = 5
HIST = 5
STEPS = ITERS - 1
SECTIONS = 8
RING = 4
N_DP = 32
ROWS = 8
PACK = RING * ROWS
TOK = RING * PACK
D = 4096
FFL = 344
FFP = 384
WIDTHS = (1024, 1024, 1024, 1024)
CHUNKS = len(WIDTHS)
STARTS = tuple(sum(WIDTHS[:c]) for c in range(CHUNKS))
NT = 512
LATER = 7.4
MESH = pl.DeviceIdType.MESH
F32 = jnp.float32
BF16 = jnp.bfloat16


def solve_small(entries, values):
    count = len(values)
    entries = [list(row) for row in entries]
    values = list(values)
    for p in range(count):
        for i in range(p + 1, count):
            factor = entries[i][p] / entries[p][p]
            for j in range(p, count):
                entries[i][j] = entries[i][j] - factor * entries[p][j]
            values[i] = values[i] - factor * values[p]
    answer = [None] * count
    for i in range(count - 1, -1, -1):
        accum = values[i]
        for j in range(i + 1, count):
            accum = accum - entries[i][j] * answer[j]
        answer[i] = accum / entries[i][i]
    return answer


def folded(value):
    total = value[:, :128]
    for t in range(1, value.shape[1] // 128):
        total = total + value[:, t * 128 : (t + 1) * 128]
    return total


def order_of_work():
    work = []
    for c in range(CHUNKS):
        at = 7.0 * (STARTS[c] + WIDTHS[c]) / D
        work += [(at, 0, c), (at + 3.9, 1, c), (at + LATER, 2, c)]
    return [(stage, c) for _, stage, c in sorted(work)]


def kernel(
    inject_ref, gain_ref, wg_hbm, wu_hbm, wd_hbm,
    iterate_ref, mixing_ref,
    wgu, wgt, eye, wd, pre, hid, images, misfits, x_ref, inj, prev, past,
    g, p, pr, q, qown, qr, osend, orecv, gsum, gmsg, grecv, gram_s, coef, cross, wts, msum, mh,
    w_local, w_send, w_recv, n_send, n_recv,
    ab_send, ab_recv, rb_send, rb_recv, rs_send, rs_recv,
    z_send, z_recv, g_send, g_recv, m_send, m_recv,
):
    sec = lax.axis_index("section")
    dp = lax.axis_index("dp")
    core = lax.rem(dp, 2)
    cx = lax.div(dp, 8)
    cy = lax.rem(lax.div(dp, 2), RING)
    small = cx + core * (cy - cx)
    big = cy + core * (cx - cy)
    step_small = 8 - 6 * core
    step_big = 2 + 6 * core
    next_sec = lax.rem(sec + 1, SECTIONS)
    last_sec = lax.rem(sec + SECTIONS - 1, SECTIONS)

    def in_small(j):
        return lax.rem(small + RING + j, RING) * step_small + big * step_big + core

    def at_big(j):
        return (sec, small * step_small + lax.rem(big + RING + j, RING) * step_big + core)

    sibling = (sec, dp + 1 - 2 * core)

    def remote(src, dst, send, recv, device):
        return pltpu.make_async_remote_copy(
            src_ref=src, dst_ref=dst, send_sem=send, recv_sem=recv, device_id=device, device_id_type=MESH
        )

    def cols(c):
        return pl.ds(STARTS[c], WIDTHS[c])

    local_copies = []
    shared_copies = []
    for c in range(CHUNKS):
        local_copies.append(
            pltpu.make_async_copy(wd_hbm.at[:, cols(c)], wd.at[pl.ds(0, FFL), cols(c)], w_local.at[2 + c])
        )
        shared_copies.append(
            remote(
                wd_hbm.at[:, cols(c)], wd.at[pl.ds(FFP, FFL), cols(c)], w_send.at[2 + c], w_recv.at[2 + c], sibling
            )
        )
    for i, ref in ((0, wg_hbm), (1, wu_hbm)):
        local_copies.append(pltpu.make_async_copy(ref, wgu.at[pl.ds(i * FFP, FFL), :], w_local.at[i]))
        shared_copies.append(
            remote(ref, wgu.at[pl.ds((2 + i) * FFP, FFL), :], w_send.at[i], w_recv.at[i], sibling)
        )
    for copy in local_copies:
        copy.start()

    barrier = pltpu.get_barrier_semaphore()

    def greet(device):
        pl.semaphore_signal(barrier, inc=1, device_id=device, device_id_type=MESH)

    @pl.loop(1, N_DP)
    def _(d):
        greet((sec, lax.rem(dp + d, N_DP)))

    for i in range(RING):
        greet((next_sec, in_small(i)))
        greet((last_sec, in_small(-i)))

    for ref in (x_ref, prev, images, misfits, past, gram_s, coef, cross, wts, mh, pre):
        ref[...] = jnp.zeros_like(ref)
    for h in range(2):
        wgu[2 * h * FFP + FFL : (2 * h + 1) * FFP, :] = jnp.zeros((FFP - FFL, D), BF16)
        wgu[(2 * h + 1) * FFP + FFL : (2 * h + 2) * FFP, :] = jnp.zeros((FFP - FFL, D), BF16)
        wd[h * FFP + FFL : (h + 1) * FFP, :] = jnp.zeros((FFP - FFL, D), BF16)
    corner = lax.broadcasted_iota(jnp.int32, (256, 256), 0) == lax.broadcasted_iota(jnp.int32, (256, 256), 1)
    eye[...] = jnp.where(corner, 1.0, 0.0).astype(BF16)
    inj[0] = inject_ref[...]

    def turn(half, start, stop):
        @pl.loop(start, stop)
        def _(n):
            at = pl.ds(pl.multiple_of(n * 256, 256), 256)
            rows = pl.ds(half * 2 * FFP, 2 * FFP)
            wgt[at, rows] = lax.dot_general(
                eye[...], wgu[rows, at], (((1,), (1,)), ((), ())), preferred_element_type=F32
            ).astype(BF16)

    def share_inject(i):
        return remote(inject_ref, inj.at[i], n_send.at[i - 1], n_recv.at[i - 1], (sec, in_small(i)))

    pl.semaphore_wait(barrier, N_DP - 1 + 2 * RING)
    for copy in shared_copies:
        copy.start()
    for i in range(1, RING):
        share_inject(i).start()

    lane = lax.broadcasted_iota(jnp.int32, (1, 128), 1)
    cells = float(ROWS * N_DP * D)

    def big_gather(c, j):
        return remote(
            g.at[0, :, cols(c)], g.at[j, :, cols(c)], ab_send.at[c, j - 1], ab_recv.at[c, j - 1], at_big(j)
        )

    def big_reduce(c, j):
        return remote(
            p.at[j, :, cols(c)], pr.at[j - 1, :, cols(c)], rb_send.at[c, j - 1], rb_recv.at[c, j - 1], at_big(-j)
        )

    def small_reduce(c, j):
        return remote(
            q.at[j - 1, :, cols(c)], qr.at[j - 1, :, cols(c)], rs_send.at[c, j - 1], rs_recv.at[c, j - 1],
            (sec, in_small(-j)),
        )

    def combine(at):
        value = wts[0] * images[0, :, at]
        for i in range(1, HIST):
            value = value + wts[i] * images[i, :, at]
        return value

    @pl.loop(0, ITERS)
    def _(k):
        parity = lax.rem(k, 2)
        going = k < STEPS

        def hand_on(c, i):
            return remote(
                osend.at[:, cols(c)], orecv.at[k, i, :, cols(c)], z_send.at[c, i], z_recv.at[k, c],
                (next_sec, in_small(i)),
            )

        def tell_norms(j):
            return remote(mh.at[k, 0], mh.at[k, j], m_send, m_recv, at_big(j))

        @pl.when(k > 0)
        def _():
            others = mh.at[k - 1, pl.ds(1, RING - 1)]
            pltpu.make_async_copy(others, others, m_recv).wait()
            pltpu.make_async_copy(others, others, m_send).wait()

        square = mh[0].reshape(TOK, 128) * cross[0]
        for l in range(1, STEPS):
            square = square + mh[l].reshape(TOK, 128) * cross[l]
        square = jnp.maximum(jnp.sum(square, axis=1, keepdims=True), 0.0)
        inverse = jnp.broadcast_to(lax.rsqrt(square / float(D) + 1e-06), (TOK, 128))

        def product_of(at):
            value = coef[0, :1] * pre[0, :, at]
            for l in range(1, STEPS):
                value = value + coef[l, :1] * pre[l, :, at]
            return value * inverse

        for h in range(2):
            for t in range(FFP // 128):
                gate = product_of(pl.ds(2 * h * FFP + t * 128, 128))
                up = product_of(pl.ds((2 * h + 1) * FFP + t * 128, 128))
                value = gate / (1.0 + jnp.exp(-gate)) * up
                real = lax.broadcasted_iota(jnp.int32, (TOK, 128), 1) < FFL - t * 128
                hid[:, h * FFP + t * 128 : h * FFP + (t + 1) * 128] = jnp.where(real, value, 0.0).astype(BF16)

        for c in range(CHUNKS):
            @pl.when(k == 0)
            def _():
                local_copies[c].wait()
                shared_copies[c].wait_recv()

            product = jnp.dot(hid[...], wd[:, cols(c)], preferred_element_type=F32).astype(BF16)
            p[:, :, cols(c)] = product.reshape(RING, PACK, WIDTHS[c])
            for j in (2, 1, 3):
                big_reduce(c, j).start()

        @pl.when(k == 0)
        def _():
            for copy in local_copies[CHUNKS:]:
                copy.wait()
            turn(0, 0, 8)

        for c in range(D // 128):
            at = pl.ds(c * 128, 128)
            x_ref[:, at] = combine(at)
        gsum[...] = jnp.zeros_like(gsum)
        msum[...] = jnp.zeros_like(msum)

        def sum_big(c):
            for j in (1, 3, 2):
                big_reduce(c, j).wait_recv()
            total = p[0, :, cols(c)].astype(F32)
            for j in range(3):
                total = total + pr[j, :, cols(c)].astype(F32)
            qown[:, cols(c)] = total[:ROWS]
            for j in (2, 1, 3):
                q[j - 1, :, cols(c)] = total[j * ROWS : (j + 1) * ROWS].astype(BF16)
                small_reduce(c, j).start()

            if c in (0, 1):
                @pl.when(k == 0)
                def _():
                    turn(0, 8 + 4 * c, 12 + 4 * c)

        def sum_small(c):
            for j in (1, 3, 2):
                small_reduce(c, j).wait_recv()
            total = qown[:, cols(c)]
            for j in range(3):
                total = total + qr[j, :, cols(c)].astype(F32)
            osend[:, cols(c)] = (x_ref[:, cols(c)] + total).astype(BF16)

            @pl.when(going)
            def _():
                for i in (2, 1, 3):
                    hand_on(c, i).start()

            hand_on(c, 0).start()
            if c == 0:
                @pl.when(k == 0)
                def _():
                    for i in range(1, RING):
                        share_inject(i).wait_recv()
                    for copy in shared_copies[CHUNKS:]:
                        copy.wait_recv()

            if c < 4:
                @pl.when(k == 0)
                def _():
                    turn(1, 4 * c, 4 * c + 4)

        def gather(c):
            @pl.when(going)
            def _():
                came = orecv.at[k, :, :, cols(c)]
                pltpu.make_async_copy(came, came, z_recv.at[k, c]).wait()

            @pl.when(k == STEPS)
            def _():
                came = orecv.at[k, 0, :, cols(c)]
                pltpu.make_async_copy(came, came, z_recv.at[k, c]).wait()

            @pl.when(going)
            def _():
                rows = []
                for i in range(RING):
                    at = pl.ds(i * ROWS, ROWS)
                    mapped = inj[i, :, cols(c)].astype(F32) + 0.5 * orecv[k, i, :, cols(c)].astype(F32)
                    step = mapped - prev[at, cols(c)]
                    prev[at, cols(c)] = mapped
                    past[k, at, cols(c)] = step
                    rows.append(step * gain_ref[:, cols(c)])
                g[0, :, cols(c)] = jnp.concatenate(rows, axis=0).astype(BF16)
                for j in (2, 1, 3):
                    big_gather(c, j).start()
                for i in range(RING):
                    at = pl.ds(i * ROWS, ROWS)
                    step = past[k, at, cols(c)]
                    for l in range(STEPS):
                        msum[l, at, :] += folded(step * past[l, at, cols(c)])

            mapped = inj[0, :, cols(c)].astype(F32) + 0.5 * orecv[k, 0, :, cols(c)].astype(F32)
            misfit = mapped - x_ref[:, cols(c)]
            images[k, :, cols(c)] = mapped
            misfits[k, :, cols(c)] = misfit
            for i in range(HIST):
                gsum[i] += folded(misfit * misfits[i, :, cols(c)])

        for stage, c in order_of_work():
            (sum_big, sum_small, gather)[stage](c)

        row = jnp.zeros((1, 128), F32)
        for i in range(HIST):
            value = jnp.sum(jnp.sum(gsum[i], axis=0, keepdims=True), axis=1, keepdims=True)
            row = jnp.where(lane == i, value, row)
        gmsg[...] = row

        @pl.loop(1, N_DP)
        def _(d):
            remote(
                gmsg, grecv.at[parity, d - 1], g_send, g_recv.at[parity], (sec, lax.rem(dp + d, N_DP))
            ).start()

        @pl.when(going)
        def _():
            table = jnp.zeros((PACK, 128), F32)
            for l in range(STEPS):
                table = jnp.where(lane == l, jnp.sum(msum[l], axis=1, keepdims=True), table)
            mh[k, 0] = table
            for j in (2, 1, 3):
                tell_norms(j).start()

        for c in range(CHUNKS):
            for j in (1, 3, 2):
                big_reduce(c, j).wait_send()
                small_reduce(c, j).wait_send()
            hand_on(c, 0).wait_send()

        @pl.when(going)
        def _():
            for c in range(CHUNKS):
                for j in (1, 3, 2):
                    big_gather(c, j).wait_recv()
                tokens = g[:, :, cols(c)].reshape(TOK, WIDTHS[c])

                @pl.loop(0, 4 * FFP // NT)
                def _(n):
                    at = pl.ds(pl.multiple_of(n * NT, NT), NT)
                    product = jnp.dot(tokens, wgt[cols(c), at], preferred_element_type=F32)
                    if c == 0:
                        pre[k, :, at] = product
                    else:
                        pre[k, :, at] += product

            for c in range(CHUNKS):
                for j in (1, 3, 2):
                    big_gather(c, j).wait_send()
                    hand_on(c, j).wait_send()

        pltpu.make_async_copy(grecv.at[parity], grecv.at[parity], g_recv.at[parity]).wait()
        row = (row + jnp.sum(grecv[parity], axis=0)) / cells
        pltpu.make_async_copy(grecv.at[parity], grecv.at[parity], g_send).wait()

        fresh = [
            jnp.broadcast_to(jnp.sum(jnp.where(lane == i, row, 0.0), axis=1, keepdims=True), (8, 128))
            for i in range(HIST)
        ]
        gram = [[None] * HIST for _ in range(HIST)]
        for i in range(HIST):
            for j in range(i + 1):
                slot = i * (i + 1) // 2 + j
                entry = jnp.where(k == i, fresh[j], gram_s[slot])
                gram_s[slot] = entry
                gram[i][j] = entry
                gram[j][i] = entry
        steps = jnp.full((8, 128), k + 1, jnp.int32)
        live = [jnp.where(steps > i, 1.0, 0.0) for i in range(HIST)]
        trace = gram[0][0]
        for i in range(1, HIST):
            trace = trace + gram[i][i]
        damp = 0.01 * trace / steps.astype(F32) + 1e-06
        system = [[gram[i][j] * live[i] * live[j] for j in range(HIST)] for i in range(HIST)]
        for i in range(HIST):
            system[i][i] = system[i][i] + (live[i] * damp + (1.0 - live[i]))
        beta = solve_small(system, live)
        whole = beta[0]
        for i in range(1, HIST):
            whole = whole + beta[i]
        weights = [value / whole for value in beta]
        mixed = jnp.zeros((1, 128), F32)
        for i in range(HIST):
            wts[i] = weights[i]
            mixed = jnp.where(lane == i, weights[i][:1], mixed)
        mixing_ref[pl.ds(k, 1), :] = mixed[:, :HIST]
        tails = [weights[HIST - 1]]
        for i in range(HIST - 2, -1, -1):
            tails.insert(0, tails[0] + weights[i])
        for l in range(STEPS):
            coef[l] = tails[l]
            line = jnp.zeros((1, 128), F32)
            for i in range(l + 1):
                line = jnp.where(lane == i, (1.0 if i == l else 2.0) * tails[l][:1] * tails[i][:1], line)
            cross[l] = line

    for copy in shared_copies:
        copy.wait_send()
    for i in range(1, RING):
        share_inject(i).wait_send()
    for c in range(D // 128):
        at = pl.ds(c * 128, 128)
        iterate_ref[:, at] = combine(at)


def local(inject, w_gate, w_up, w_down, gain):
    vmem = pl.BlockSpec(memory_space=pltpu.VMEM)
    hbm = pl.BlockSpec(memory_space=pl.ANY)
    dma = pltpu.SemaphoreType.DMA
    iterate, mixing = pl.pallas_call(
        kernel,
        out_shape=(jax.ShapeDtypeStruct((ROWS, D), F32), jax.ShapeDtypeStruct((ITERS, HIST), F32)),
        in_specs=[vmem, vmem, hbm, hbm, hbm],
        out_specs=(vmem, vmem),
        scratch_shapes=[
            pltpu.VMEM((4 * FFP, D), BF16),
            pltpu.VMEM((D, 4 * FFP), BF16),
            pltpu.VMEM((256, 256), BF16),
            pltpu.VMEM((2 * FFP, D), BF16),
            pltpu.VMEM((STEPS, TOK, 4 * FFP), F32),
            pltpu.VMEM((TOK, 2 * FFP), BF16),
            pltpu.VMEM((HIST, ROWS, D), F32),
            pltpu.VMEM((HIST, ROWS, D), F32),
            pltpu.VMEM((ROWS, D), F32),
            pltpu.VMEM((RING, ROWS, D), BF16),
            pltpu.VMEM((PACK, D), F32),
            pltpu.VMEM((STEPS, PACK, D), F32),
            pltpu.VMEM((RING, PACK, D), BF16),
            pltpu.VMEM((RING, PACK, D), BF16),
            pltpu.VMEM((3, PACK, D), BF16),
            pltpu.VMEM((3, ROWS, D), BF16),
            pltpu.VMEM((ROWS, D), F32),
            pltpu.VMEM((3, ROWS, D), BF16),
            pltpu.VMEM((ROWS, D), BF16),
            pltpu.VMEM((ITERS, RING, ROWS, D), BF16),
            pltpu.VMEM((HIST, ROWS, 128), F32),
            pltpu.VMEM((1, 128), F32),
            pltpu.VMEM((2, N_DP - 1, 1, 128), F32),
            pltpu.VMEM((HIST * (HIST + 1) // 2, 8, 128), F32),
            pltpu.VMEM((STEPS, 8, 128), F32),
            pltpu.VMEM((STEPS, 1, 128), F32),
            pltpu.VMEM((HIST, 8, 128), F32),
            pltpu.VMEM((STEPS, PACK, 128), F32),
            pltpu.VMEM((STEPS, RING, PACK, 128), F32),
            dma((2 + CHUNKS,)), dma((2 + CHUNKS,)), dma((2 + CHUNKS,)), dma((3,)), dma((3,)),
            dma((CHUNKS, 3)), dma((CHUNKS, 3)), dma((CHUNKS, 3)), dma((CHUNKS, 3)), dma((CHUNKS, 3)), dma((CHUNKS, 3)),
            dma((CHUNKS, RING)), dma((ITERS, CHUNKS)), dma, dma((2,)), dma, dma,
        ],
        compiler_params=pltpu.CompilerParams(
            collective_id=0, has_side_effects=True, vmem_limit_bytes=62 * 1024 * 1024
        ),
    )(inject[0], gain, w_gate[0].T, w_up[0].T, w_down[0])
    return iterate[None], mixing[None]


def solution(mesh):
    return jax.shard_map(
        local,
        mesh=mesh,
        in_specs=(
            P("section", "dp", None),
            P("section", None, "dp"),
            P("section", None, "dp"),
            P("section", "dp", None),
            P("section", None),
        ),
        out_specs=(P("section", "dp", None), P("section", None, None)),
        check_vma=False,
    )
```

```python
import jax
import jax.numpy as jnp
from jax import lax
from jax.experimental import pallas as pl
from jax.experimental.pallas import tpu as pltpu
from jax.sharding import PartitionSpec as P

ITERS = 5
HIST = 5
STEPS = ITERS - 1
SECTIONS = 8
RING = 4
N_DP = 32
ROWS = 8
PACK = RING * ROWS
TOK = RING * PACK
D = 4096
FFL = 344
FFP = 384
WIDTHS = (1024, 1024, 1024, 512, 512)
CHUNKS = len(WIDTHS)
STARTS = tuple(sum(WIDTHS[:c]) for c in range(CHUNKS))
NT = 1536
LATER = 7.4
FAR_FIRST = [(i, j, l) for i in (2, 1, 3, 0) for j in (2, 1, 3, 0) for l in (1, 0)][:-1]
MESH = pl.DeviceIdType.MESH
F32 = jnp.float32
BF16 = jnp.bfloat16


def solve_small(entries, values):
    count = len(values)
    entries = [list(row) for row in entries]
    values = list(values)
    for p in range(count):
        for i in range(p + 1, count):
            factor = entries[i][p] / entries[p][p]
            for j in range(p, count):
                entries[i][j] = entries[i][j] - factor * entries[p][j]
            values[i] = values[i] - factor * values[p]
    answer = [None] * count
    for i in range(count - 1, -1, -1):
        accum = values[i]
        for j in range(i + 1, count):
            accum = accum - entries[i][j] * answer[j]
        answer[i] = accum / entries[i][i]
    return answer


def folded(value):
    total = value[:, :128]
    for t in range(1, value.shape[1] // 128):
        total = total + value[:, t * 128 : (t + 1) * 128]
    return total


def order_of_work():
    work = []
    for c in range(CHUNKS):
        at = 7.0 * (STARTS[c] + WIDTHS[c]) / D
        work += [(at, 0, c), (at + 3.9, 1, c), (at + LATER, 2, c), (at + 12.0, 3, c)]
    return [(stage, c) for _, stage, c in sorted(work)]


def kernel(
    inject_ref, gain_ref, wg_hbm, wu_hbm, wd_hbm,
    iterate_ref, mixing_ref,
    wgu, wgt, eye, wd, pre, hid, images, misfits, x_ref, inj, prev, past,
    g, p, pr, q, qown, qr, osend, orecv, gsum, gmsg, grecv, gram_s, coef, cross, wts, msum, mh,
    w_local, w_send, w_recv, n_send, n_recv,
    ab_send, ab_recv, rb_send, rb_recv, rs_send, rs_recv,
    z_send, z_recv, g_send, g_recv, m_send, m_recv,
):
    sec = lax.axis_index("section")
    dp = lax.axis_index("dp")
    core = lax.rem(dp, 2)
    cx = lax.div(dp, 8)
    cy = lax.rem(lax.div(dp, 2), RING)
    small = cx + core * (cy - cx)
    big = cy + core * (cx - cy)
    step_small = 8 - 6 * core
    step_big = 2 + 6 * core
    next_sec = lax.rem(sec + 1, SECTIONS)
    last_sec = lax.rem(sec + SECTIONS - 1, SECTIONS)

    def in_small(j):
        return lax.rem(small + RING + j, RING) * step_small + big * step_big + core

    def at_big(j):
        return (sec, small * step_small + lax.rem(big + RING + j, RING) * step_big + core)

    sibling = (sec, dp + 1 - 2 * core)

    def remote(src, dst, send, recv, device):
        return pltpu.make_async_remote_copy(
            src_ref=src, dst_ref=dst, send_sem=send, recv_sem=recv, device_id=device, device_id_type=MESH
        )

    def cols(c):
        return pl.ds(STARTS[c], WIDTHS[c])

    local_copies = []
    shared_copies = []
    for c in range(CHUNKS):
        local_copies.append(
            pltpu.make_async_copy(wd_hbm.at[:, cols(c)], wd.at[pl.ds(0, FFL), cols(c)], w_local.at[2 + c])
        )
        shared_copies.append(
            remote(
                wd_hbm.at[:, cols(c)], wd.at[pl.ds(FFP, FFL), cols(c)], w_send.at[2 + c], w_recv.at[2 + c], sibling
            )
        )
    for i, ref in ((0, wg_hbm), (1, wu_hbm)):
        local_copies.append(pltpu.make_async_copy(ref, wgu.at[pl.ds(i * FFP, FFL), :], w_local.at[i]))
        shared_copies.append(
            remote(ref, wgu.at[pl.ds((2 + i) * FFP, FFL), :], w_send.at[i], w_recv.at[i], sibling)
        )
    for copy in local_copies:
        copy.start()

    barrier = pltpu.get_barrier_semaphore()

    def greet(device):
        pl.semaphore_signal(barrier, inc=1, device_id=device, device_id_type=MESH)

    @pl.loop(1, N_DP)
    def _(d):
        greet((sec, lax.rem(dp + d, N_DP)))

    for i in range(RING):
        greet((next_sec, in_small(i)))
        greet((last_sec, in_small(-i)))

    for ref in (x_ref, prev, images, misfits, past, gram_s, coef, cross, wts, mh, pre):
        ref[...] = jnp.zeros_like(ref)
    for h in range(2):
        wgu[2 * h * FFP + FFL : (2 * h + 1) * FFP, :] = jnp.zeros((FFP - FFL, D), BF16)
        wgu[(2 * h + 1) * FFP + FFL : (2 * h + 2) * FFP, :] = jnp.zeros((FFP - FFL, D), BF16)
        wd[h * FFP + FFL : (h + 1) * FFP, :] = jnp.zeros((FFP - FFL, D), BF16)
    corner = lax.broadcasted_iota(jnp.int32, (256, 256), 0) == lax.broadcasted_iota(jnp.int32, (256, 256), 1)
    eye[...] = jnp.where(corner, 1.0, 0.0).astype(BF16)
    inj[0] = inject_ref[...]

    def turn(half, start, stop):
        @pl.loop(start, stop)
        def _(n):
            at = pl.ds(pl.multiple_of(n * 256, 256), 256)
            rows = pl.ds(half * 2 * FFP, 2 * FFP)
            wgt[at, rows] = lax.dot_general(
                eye[...], wgu[rows, at], (((1,), (1,)), ((), ())), preferred_element_type=F32
            ).astype(BF16)

    def share_inject(i):
        return remote(inject_ref, inj.at[i], n_send.at[i - 1], n_recv.at[i - 1], (sec, in_small(i)))

    pl.semaphore_wait(barrier, N_DP - 1 + 2 * RING)
    for copy in shared_copies:
        copy.start()
    for i in range(1, RING):
        share_inject(i).start()

    lane = lax.broadcasted_iota(jnp.int32, (1, 128), 1)
    cells = float(ROWS * N_DP * D)

    def big_gather(c, j):
        return remote(
            g.at[0, :, cols(c)], g.at[j, :, cols(c)], ab_send.at[c, j - 1], ab_recv.at[c, j - 1], at_big(j)
        )

    def big_reduce(c, j):
        return remote(
            p.at[j, :, cols(c)], pr.at[j - 1, :, cols(c)], rb_send.at[c, j - 1], rb_recv.at[c, j - 1], at_big(-j)
        )

    def small_reduce(c, j):
        return remote(
            q.at[j - 1, :, cols(c)], qr.at[j - 1, :, cols(c)], rs_send.at[c, j - 1], rs_recv.at[c, j - 1],
            (sec, in_small(-j)),
        )

    def combine(at):
        value = wts[0] * images[0, :, at]
        for i in range(1, HIST):
            value = value + wts[i] * images[i, :, at]
        return value

    @pl.loop(0, ITERS)
    def _(k):
        parity = lax.rem(k, 2)
        going = k < STEPS

        def hand_on(c, i):
            return remote(
                osend.at[:, cols(c)], orecv.at[k, i, :, cols(c)], z_send.at[c, i], z_recv.at[k, c],
                (next_sec, in_small(i)),
            )

        def tell_norms(j):
            return remote(mh.at[k, 0], mh.at[k, j], m_send, m_recv, at_big(j))

        @pl.when(k > 0)
        def _():
            others = mh.at[k - 1, pl.ds(1, RING - 1)]
            pltpu.make_async_copy(others, others, m_recv).wait()
            pltpu.make_async_copy(others, others, m_send).wait()

        square = mh[0].reshape(TOK, 128) * cross[0]
        for l in range(1, STEPS):
            square = square + mh[l].reshape(TOK, 128) * cross[l]
        square = jnp.maximum(jnp.sum(square, axis=1, keepdims=True), 0.0)
        inverse = jnp.broadcast_to(lax.rsqrt(square / float(D) + 1e-06), (TOK, 128))

        def product_of(at):
            value = coef[0, :1] * pre[0, :, at]
            for l in range(1, STEPS):
                value = value + coef[l, :1] * pre[l, :, at]
            return value * inverse

        for h in range(2):
            for t in range(FFP // 128):
                gate = product_of(pl.ds(2 * h * FFP + t * 128, 128))
                up = product_of(pl.ds((2 * h + 1) * FFP + t * 128, 128))
                value = gate / (1.0 + jnp.exp(-gate)) * up
                real = lax.broadcasted_iota(jnp.int32, (TOK, 128), 1) < FFL - t * 128
                hid[:, h * FFP + t * 128 : h * FFP + (t + 1) * 128] = jnp.where(real, value, 0.0).astype(BF16)

        for c in range(CHUNKS):
            @pl.when(k == 0)
            def _():
                local_copies[c].wait()
                shared_copies[c].wait_recv()

            product = jnp.dot(hid[...], wd[:, cols(c)], preferred_element_type=F32).astype(BF16)
            p[:, :, cols(c)] = product.reshape(RING, PACK, WIDTHS[c])
            for j in (2, 1, 3):
                big_reduce(c, j).start()

        @pl.when(k == 0)
        def _():
            for copy in local_copies[CHUNKS:]:
                copy.wait()
            turn(0, 0, 8)

        for c in range(D // 128):
            at = pl.ds(c * 128, 128)
            x_ref[:, at] = combine(at)
        gsum[...] = jnp.zeros_like(gsum)
        msum[...] = jnp.zeros_like(msum)

        def sum_big(c):
            for j in (1, 3, 2):
                big_reduce(c, j).wait_recv()
            total = p[0, :, cols(c)].astype(F32)
            for j in range(3):
                total = total + pr[j, :, cols(c)].astype(F32)
            qown[:, cols(c)] = total[:ROWS]
            for j in (2, 1, 3):
                q[j - 1, :, cols(c)] = total[j * ROWS : (j + 1) * ROWS].astype(BF16)
                small_reduce(c, j).start()

            if c in (0, 1):
                @pl.when(k == 0)
                def _():
                    turn(0, 8 + 4 * c, 12 + 4 * c)

        def sum_small(c):
            for j in (1, 3, 2):
                small_reduce(c, j).wait_recv()
            total = qown[:, cols(c)]
            for j in range(3):
                total = total + qr[j, :, cols(c)].astype(F32)
            osend[:, cols(c)] = (x_ref[:, cols(c)] + total).astype(BF16)

            @pl.when(going)
            def _():
                for i in (2, 1, 3):
                    hand_on(c, i).start()

            hand_on(c, 0).start()
            if c == 0:
                @pl.when(k == 0)
                def _():
                    for i in range(1, RING):
                        share_inject(i).wait_recv()
                    for copy in shared_copies[CHUNKS:]:
                        copy.wait_recv()

            if c < 4:
                @pl.when(k == 0)
                def _():
                    turn(1, 4 * c, 4 * c + 4)

        def gather(c):
            @pl.when(going)
            def _():
                came = orecv.at[k, :, :, cols(c)]
                pltpu.make_async_copy(came, came, z_recv.at[k, c]).wait()

            @pl.when(k == STEPS)
            def _():
                came = orecv.at[k, 0, :, cols(c)]
                pltpu.make_async_copy(came, came, z_recv.at[k, c]).wait()

            @pl.when(going)
            def _():
                rows = []
                for i in range(RING):
                    at = pl.ds(i * ROWS, ROWS)
                    mapped = inj[i, :, cols(c)].astype(F32) + 0.5 * orecv[k, i, :, cols(c)].astype(F32)
                    step = mapped - prev[at, cols(c)]
                    prev[at, cols(c)] = mapped
                    past[k, at, cols(c)] = step
                    rows.append(step * gain_ref[:, cols(c)])
                g[0, :, cols(c)] = jnp.concatenate(rows, axis=0).astype(BF16)
                for j in (2, 1, 3):
                    big_gather(c, j).start()
                for i in range(RING):
                    at = pl.ds(i * ROWS, ROWS)
                    step = past[k, at, cols(c)]
                    for l in range(STEPS):
                        msum[l, at, :] += folded(step * past[l, at, cols(c)])

            mapped = inj[0, :, cols(c)].astype(F32) + 0.5 * orecv[k, 0, :, cols(c)].astype(F32)
            misfit = mapped - x_ref[:, cols(c)]
            images[k, :, cols(c)] = mapped
            misfits[k, :, cols(c)] = misfit
            for i in range(HIST):
                gsum[i] += folded(misfit * misfits[i, :, cols(c)])

        def multiply(c):
            @pl.when(going)
            def _():
                for j in (1, 3, 2):
                    big_gather(c, j).wait_recv()
                tokens = g[:, :, cols(c)].reshape(TOK, WIDTHS[c])

                @pl.loop(0, 4 * FFP // NT)
                def _(n):
                    at = pl.ds(pl.multiple_of(n * NT, NT), NT)
                    product = jnp.dot(tokens, wgt[cols(c), at], preferred_element_type=F32)
                    if c == 0:
                        pre[k, :, at] = product
                    else:
                        pre[k, :, at] += product

        def tell():
            row = jnp.zeros((1, 128), F32)
            for i in range(HIST):
                value = jnp.sum(jnp.sum(gsum[i], axis=0, keepdims=True), axis=1, keepdims=True)
                row = jnp.where(lane == i, value, row)
            gmsg[...] = row

            for n, (i, j, l) in enumerate(FAR_FIRST):
                x, y, other = lax.rem(cx + i, RING), lax.rem(cy + j, RING), lax.rem(core + l, 2)
                remote(
                    gmsg, grecv.at[parity, n], g_send, g_recv.at[parity], (sec, x * 8 + y * 2 + other)
                ).start()

            @pl.when(going)
            def _():
                table = jnp.zeros((PACK, 128), F32)
                for l in range(STEPS):
                    table = jnp.where(lane == l, jnp.sum(msum[l], axis=1, keepdims=True), table)
                mh[k, 0] = table
                for j in (2, 1, 3):
                    tell_norms(j).start()

        for stage, c in order_of_work():
            (sum_big, sum_small, gather, multiply)[stage](c)
            if stage == 2 and c == CHUNKS - 1:
                tell()

        for c in range(CHUNKS):
            for j in (1, 3, 2):
                big_reduce(c, j).wait_send()
                small_reduce(c, j).wait_send()
            hand_on(c, 0).wait_send()

        @pl.when(going)
        def _():
            for c in range(CHUNKS):
                for j in (1, 3, 2):
                    big_gather(c, j).wait_send()
                    hand_on(c, j).wait_send()

        pltpu.make_async_copy(grecv.at[parity], grecv.at[parity], g_recv.at[parity]).wait()
        row = (gmsg[...] + jnp.sum(grecv[parity], axis=0)) / cells
        pltpu.make_async_copy(grecv.at[parity], grecv.at[parity], g_send).wait()

        fresh = [
            jnp.broadcast_to(jnp.sum(jnp.where(lane == i, row, 0.0), axis=1, keepdims=True), (8, 128))
            for i in range(HIST)
        ]
        gram = [[None] * HIST for _ in range(HIST)]
        for i in range(HIST):
            for j in range(i + 1):
                slot = i * (i + 1) // 2 + j
                entry = jnp.where(k == i, fresh[j], gram_s[slot])
                gram_s[slot] = entry
                gram[i][j] = entry
                gram[j][i] = entry
        steps = jnp.full((8, 128), k + 1, jnp.int32)
        live = [jnp.where(steps > i, 1.0, 0.0) for i in range(HIST)]
        trace = gram[0][0]
        for i in range(1, HIST):
            trace = trace + gram[i][i]
        damp = 0.01 * trace / steps.astype(F32) + 1e-06
        system = [[gram[i][j] * live[i] * live[j] for j in range(HIST)] for i in range(HIST)]
        for i in range(HIST):
            system[i][i] = system[i][i] + (live[i] * damp + (1.0 - live[i]))
        beta = solve_small(system, live)
        whole = beta[0]
        for i in range(1, HIST):
            whole = whole + beta[i]
        weights = [value / whole for value in beta]
        mixed = jnp.zeros((1, 128), F32)
        for i in range(HIST):
            wts[i] = weights[i]
            mixed = jnp.where(lane == i, weights[i][:1], mixed)
        mixing_ref[pl.ds(k, 1), :] = mixed[:, :HIST]
        tails = [weights[HIST - 1]]
        for i in range(HIST - 2, -1, -1):
            tails.insert(0, tails[0] + weights[i])
        for l in range(STEPS):
            coef[l] = tails[l]
            line = jnp.zeros((1, 128), F32)
            for i in range(l + 1):
                line = jnp.where(lane == i, (1.0 if i == l else 2.0) * tails[l][:1] * tails[i][:1], line)
            cross[l] = line

    for copy in shared_copies:
        copy.wait_send()
    for i in range(1, RING):
        share_inject(i).wait_send()
    for c in range(D // 128):
        at = pl.ds(c * 128, 128)
        iterate_ref[:, at] = combine(at)


def local(inject, w_gate, w_up, w_down, gain):
    vmem = pl.BlockSpec(memory_space=pltpu.VMEM)
    hbm = pl.BlockSpec(memory_space=pl.ANY)
    dma = pltpu.SemaphoreType.DMA
    iterate, mixing = pl.pallas_call(
        kernel,
        out_shape=(jax.ShapeDtypeStruct((ROWS, D), F32), jax.ShapeDtypeStruct((ITERS, HIST), F32)),
        in_specs=[vmem, vmem, hbm, hbm, hbm],
        out_specs=(vmem, vmem),
        scratch_shapes=[
            pltpu.VMEM((4 * FFP, D), BF16),
            pltpu.VMEM((D, 4 * FFP), BF16),
            pltpu.VMEM((256, 256), BF16),
            pltpu.VMEM((2 * FFP, D), BF16),
            pltpu.VMEM((STEPS, TOK, 4 * FFP), F32),
            pltpu.VMEM((TOK, 2 * FFP), BF16),
            pltpu.VMEM((HIST, ROWS, D), F32),
            pltpu.VMEM((HIST, ROWS, D), F32),
            pltpu.VMEM((ROWS, D), F32),
            pltpu.VMEM((RING, ROWS, D), BF16),
            pltpu.VMEM((PACK, D), F32),
            pltpu.VMEM((STEPS, PACK, D), F32),
            pltpu.VMEM((RING, PACK, D), BF16),
            pltpu.VMEM((RING, PACK, D), BF16),
            pltpu.VMEM((3, PACK, D), BF16),
            pltpu.VMEM((3, ROWS, D), BF16),
            pltpu.VMEM((ROWS, D), F32),
            pltpu.VMEM((3, ROWS, D), BF16),
            pltpu.VMEM((ROWS, D), BF16),
            pltpu.VMEM((ITERS, RING, ROWS, D), BF16),
            pltpu.VMEM((HIST, ROWS, 128), F32),
            pltpu.VMEM((1, 128), F32),
            pltpu.VMEM((2, N_DP - 1, 1, 128), F32),
            pltpu.VMEM((HIST * (HIST + 1) // 2, 8, 128), F32),
            pltpu.VMEM((STEPS, 8, 128), F32),
            pltpu.VMEM((STEPS, 1, 128), F32),
            pltpu.VMEM((HIST, 8, 128), F32),
            pltpu.VMEM((STEPS, PACK, 128), F32),
            pltpu.VMEM((STEPS, RING, PACK, 128), F32),
            dma((2 + CHUNKS,)), dma((2 + CHUNKS,)), dma((2 + CHUNKS,)), dma((3,)), dma((3,)),
            dma((CHUNKS, 3)), dma((CHUNKS, 3)), dma((CHUNKS, 3)), dma((CHUNKS, 3)), dma((CHUNKS, 3)), dma((CHUNKS, 3)),
            dma((CHUNKS, RING)), dma((ITERS, CHUNKS)), dma, dma((2,)), dma, dma,
        ],
        compiler_params=pltpu.CompilerParams(
            collective_id=0, has_side_effects=True, vmem_limit_bytes=62 * 1024 * 1024
        ),
    )(inject[0], gain, w_gate[0].T, w_up[0].T, w_down[0])
    return iterate[None], mixing[None]


def solution(mesh):
    return jax.shard_map(
        local,
        mesh=mesh,
        in_specs=(
            P("section", "dp", None),
            P("section", None, "dp"),
            P("section", None, "dp"),
            P("section", "dp", None),
            P("section", None),
        ),
        out_specs=(P("section", "dp", None), P("section", None, None)),
        check_vma=False,
    )
```
